16 devices in a mesh: dz: 2 (over z), dy: 2 (over y), dx: 4 (over x, core).
Axes of the slice: x: 2, y: 2, z: 2, core: 2. Of those that a mesh axis runs over, the one named last changes fastest.
Arguments:
- x_tokens: bfloat16 [65536, 1024], P(('dz', 'dy', 'dx'))
- g_tokens: bfloat16 [65536, 1024], P(('dz', 'dy', 'dx'))
- w_one: bfloat16 [1024, 4096], replicated
- w_two: bfloat16 [4096, 1024], replicated
- w_three: bfloat16 [1024, 4096], replicated
- w_four: bfloat16 [4096, 1024], replicated
- clip_norm: float32 [1], replicated
Outputs:
- output 1: float32 [1024, 4096], replicated
- output 2: float32 [4096, 1024], replicated
- output 3: float32 [1024, 4096], replicated
- output 4: float32 [4096, 1024], replicated
- output 5: bfloat16 [65536, 1024], P(('dz', 'dy', 'dx'))
All inputs are finite; a program needn't handle non-finite values.
Results may differ from the reference program's by a relative error of at most 0.0114068.
Values are sent between devices in bfloat16 or wider.
A program may use at most 1 GiB of HBM per device.

```python
import math
import jax
import jax.numpy as jnp
from jax import lax

D_MODEL = 1024
D_FF = 4096
TOKENS_DEV = 4096
NUM_DEVICES = 16

TOKENS = TOKENS_DEV * NUM_DEVICES
CLIP_BASE = math.sqrt(TOKENS_DEV * D_MODEL * D_FF / NUM_DEVICES)


def setup_inputs(seed: int = 0) -> dict:
    root_key = jax.random.key(seed)
    sub_keys = jax.random.split(root_key, 7)
    x_tokens = jax.random.normal(sub_keys[0], (TOKENS, D_MODEL), jnp.float32).astype(jnp.bfloat16)
    g_tokens = jax.random.normal(sub_keys[1], (TOKENS, D_MODEL), jnp.float32).astype(jnp.bfloat16)
    w_one = (jax.random.normal(sub_keys[2], (D_MODEL, D_FF), jnp.float32) * D_MODEL ** -0.5).astype(jnp.bfloat16)
    w_two = (jax.random.normal(sub_keys[3], (D_FF, D_MODEL), jnp.float32) * D_FF ** -0.5).astype(jnp.bfloat16)
    w_three = (jax.random.normal(sub_keys[4], (D_MODEL, D_FF), jnp.float32) * D_MODEL ** -0.5).astype(jnp.bfloat16)
    w_four = (jax.random.normal(sub_keys[5], (D_FF, D_MODEL), jnp.float32) * D_FF ** -0.5).astype(jnp.bfloat16)
    clip_norm = jax.random.uniform(sub_keys[6], (1,), jnp.float32, 0.1, 0.35) * CLIP_BASE
    return {'x_tokens': x_tokens, 'g_tokens': g_tokens, 'w_one': w_one, 'w_two': w_two, 'w_three': w_three, 'w_four': w_four, 'clip_norm': clip_norm}


def gelu_back(pre_act, upstream):
    gelu_out, gelu_pull = jax.vjp(jax.nn.gelu, pre_act.astype(jnp.float32))
    return gelu_pull(upstream.astype(jnp.float32))[0].astype(jnp.bfloat16)


def block_grads(x_rows, g_rows, w_one, w_two, w_three, w_four):
    a_one = jnp.dot(x_rows, w_one, preferred_element_type=jnp.float32).astype(jnp.bfloat16)
    h_one = jax.nn.gelu(a_one.astype(jnp.float32)).astype(jnp.bfloat16)
    h_two = (jnp.dot(h_one, w_two, preferred_element_type=jnp.float32) + x_rows.astype(jnp.float32)).astype(jnp.bfloat16)
    a_three = jnp.dot(h_two, w_three, preferred_element_type=jnp.float32).astype(jnp.bfloat16)
    h_three = jax.nn.gelu(a_three.astype(jnp.float32)).astype(jnp.bfloat16)
    grad_four = jnp.dot(h_three.T, g_rows, preferred_element_type=jnp.float32)
    dh_three = jnp.dot(g_rows, w_four.T, preferred_element_type=jnp.float32).astype(jnp.bfloat16)
    da_three = gelu_back(a_three, dh_three)
    grad_three = jnp.dot(h_two.T, da_three, preferred_element_type=jnp.float32)
    dh_two = (jnp.dot(da_three, w_three.T, preferred_element_type=jnp.float32) + g_rows.astype(jnp.float32)).astype(jnp.bfloat16)
    grad_two = jnp.dot(h_one.T, dh_two, preferred_element_type=jnp.float32)
    dh_one = jnp.dot(dh_two, w_two.T, preferred_element_type=jnp.float32).astype(jnp.bfloat16)
    da_one = gelu_back(a_one, dh_one)
    grad_one = jnp.dot(x_rows.T, da_one, preferred_element_type=jnp.float32)
    dx_rows = (jnp.dot(da_one, w_one.T, preferred_element_type=jnp.float32) + dh_two.astype(jnp.float32)).astype(jnp.bfloat16)
    return (grad_one, grad_two, grad_three, grad_four), dx_rows


def reference(x_tokens, g_tokens, w_one, w_two, w_three, w_four, clip_norm):
    x_blocks = x_tokens.reshape(NUM_DEVICES, TOKENS_DEV, D_MODEL)
    g_blocks = g_tokens.reshape(NUM_DEVICES, TOKENS_DEV, D_MODEL)

    def scan_step(grad_sums, row_pair):
        layer_grads, dx_rows = block_grads(row_pair[0], row_pair[1], w_one, w_two, w_three, w_four)
        new_sums = tuple(running_sum + block_grad for running_sum, block_grad in zip(grad_sums, layer_grads))
        return new_sums, dx_rows

    zero_init = (jnp.zeros((D_MODEL, D_FF), jnp.float32), jnp.zeros((D_FF, D_MODEL), jnp.float32), jnp.zeros((D_MODEL, D_FF), jnp.float32), jnp.zeros((D_FF, D_MODEL), jnp.float32))
    grad_sums, dx_blocks = lax.scan(scan_step, zero_init, (x_blocks, g_blocks))
    mean_grads = [layer_sum / NUM_DEVICES for layer_sum in grad_sums]
    total_sq = sum(jnp.sum(layer_mean * layer_mean) for layer_mean in mean_grads)
    clip_scale = jnp.minimum(1.0, clip_norm[0] / jnp.sqrt(total_sq))
    return (mean_grads[0] * clip_scale, mean_grads[1] * clip_scale, mean_grads[2] * clip_scale, mean_grads[3] * clip_scale, dx_blocks.reshape(TOKENS, D_MODEL))
```

```python
import functools
import math

import jax
import jax.numpy as jnp
from jax import lax
from jax.experimental import pallas as pl
from jax.experimental.pallas import tpu as pltpu
from jax.sharding import PartitionSpec as P

F32 = jnp.float32
BF16 = jnp.bfloat16
MESH = pl.DeviceIdType.MESH
AXES = ('dz', 'dy', 'dx')
ROOT = math.sqrt(2 / math.pi)
CUBE = ROOT * 0.044715

TOK = 4096
DM = 1024
DF = 4096
BC = 256
STEPS = DF // BC
BLOCKS = 2 * STEPS
MC = 1024
NCH = TOK // MC
EC = 32
NS = 6
ROWS = (DM, BC)
COLS = (BC, DM)


def nn(a, b):
    return jnp.dot(a, b, preferred_element_type=F32)


def nt(a, b):
    return lax.dot_general(a, b, (((1,), (1,)), ((), ())), preferred_element_type=F32)


def tn(a, b):
    return lax.dot_general(a, b, (((0,), (0,)), ((), ())), preferred_element_type=F32)


def gelu_pair(pre, up):
    x = pre.astype(F32)
    sq = x * x
    h = 0.5 * jnp.tanh(x * (ROOT + CUBE * sq)) + 0.5
    g = x * h
    slope = h + g * (1.0 - h) * (2 * ROOT + 6 * CUBE * sq)
    return g.astype(BF16), (up.astype(F32) * slope).astype(BF16)


def main_kernel(p0, p1, q0, wf0, wf1, wb0, wb1,
                ta, tb, dx_out, sq_out,
                pv, qv, acc, wf, wb, av, hv, gv, dv,
                own_a, own_b, r0a, r0b, r1a, r1b, r2a, r2b, r3a, r3b, sqv, sqr,
                ssem, rsem, lsem, wsem, psem, nsend, nrecv):
    own = (own_a, own_b)
    r0 = (r0a, r0b)
    r1 = (r1a, r1b)
    r2 = (r2a, r2b)
    r3 = (r3a, r3b)
    zb = lax.axis_index('dz')
    yb = lax.axis_index('dy')
    dxi = lax.axis_index('dx')
    xb = dxi // 2
    cb = dxi % 2
    partner = (zb, yb, 2 * xb + (1 - cb))

    def along(d):
        e0 = (1 - d) * (2 - d) // 2
        e1 = d * (2 - d)
        e2 = d * (d - 1) // 2
        bit = e0 * xb + e1 * yb + e2 * zb
        peer = (zb + e2 * (1 - 2 * zb), yb + e1 * (1 - 2 * yb), 2 * (xb + e0 * (1 - 2 * xb)) + cb)
        return bit, peer

    def route(i, u):
        d1 = (i + u + 2 * cb) % 3
        return along(d1), along((d1 + 1) % 3), along((d1 + 2) % 3)

    def remote(src, dst, stage, u, i, peer):
        s = i % NS
        return pltpu.make_async_remote_copy(
            src_ref=src, dst_ref=dst, send_sem=ssem.at[stage, u, s], recv_sem=rsem.at[stage, u, s],
            device_id=peer, device_id_type=MESH)

    def part(ref, slot, start, size):
        return ref.at[slot, pl.ds(pl.multiple_of(start, 16), size)]

    def load(ref, slot, start, size):
        return ref[slot, pl.ds(pl.multiple_of(start, 16), size), :]

    def region(u, i, start, size):
        ph = i // STEPS
        at = (i % STEPS) * BC
        if u == 0:
            return ta.at[ph, pl.ds(pl.multiple_of(start, 16), size), pl.ds(pl.multiple_of(at, BC), BC)]
        return tb.at[ph, pl.ds(pl.multiple_of(at + start, 16), size), :]

    def pair_copy(u, i):
        half = ROWS[u] // 2
        return remote(part(own[u], i % 2, (1 - cb) * half, half), r0[u].at[i % 3], 0, u, i, partner)

    def scatter_copy(k, u, i):
        (bits) = route(i, u)
        bit, peer = bits[k - 1]
        size = ROWS[u] // (2 << k)
        src = (r0, r1, r2)[k - 1][u]
        dst = (r1, r2, r3)[k - 1][u]
        slot = i % 3 if k == 1 else i % NS
        return remote(part(src, slot, (1 - bit) * size, size), dst.at[i % NS], k, u, i, peer)

    def offsets(u, i):
        (b1, _), (b2, _), (b3, _) = route(i, u)
        r = ROWS[u]
        oc = cb * (r // 2)
        o1 = oc + b1 * (r // 4)
        o2 = o1 + b2 * (r // 8)
        return oc, o1, o2, o2 + b3 * (r // 16)

    def gather_copy(k, u, i):
        oc, o1, o2, o3 = offsets(u, i)
        r = ROWS[u]
        way = route(i, u)
        if k == 4:
            return remote(r3[u].at[i % NS], region(u, i, o3, r // 16), k, u, i, way[2][1])
        start, size, peer = {5: (o2, r // 8, way[1][1]), 6: (o1, r // 4, way[0][1]), 7: (oc, r // 2, partner)}[k]
        return remote(region(u, i, start, size), region(u, i, start, size), k, u, i, peer)

    def keep_copy(u, i):
        o3 = offsets(u, i)[3]
        return pltpu.make_async_copy(r3[u].at[i % NS], region(u, i, o3, ROWS[u] // 16), lsem.at[u, i % NS])

    def h_pair(i):
        for u in range(2):
            pair_copy(u, i).start()

    def h_scatter1(i):
        for u in range(2):
            pair_copy(u, i).wait()
            half = ROWS[u] // 2
            r0[u][i % 3] += load(own[u], i % 2, cb * half, half)
            scatter_copy(1, u, i).start()

    def h_scatter(k, i):
        for u in range(2):
            scatter_copy(k - 1, u, i).wait()
            bit = route(i, u)[k - 2][0]
            size = ROWS[u] // (1 << k)
            src = (r0, r1)[k - 2][u]
            dst = (r1, r2)[k - 2][u]
            slot = i % 3 if k == 2 else i % NS
            dst[i % NS] += load(src, slot, bit * size, size)
            scatter_copy(k, u, i).start()

    def h_final(i):
        for u in range(2):
            scatter_copy(3, u, i).wait()
            bit = route(i, u)[2][0]
            size = ROWS[u] // 16
            tot = r3[u][i % NS] + load(r2[u], i % NS, bit * size, size)
            r3[u][i % NS] = tot
            t2 = jnp.square(tot * (1.0 / 16))
            s = jnp.zeros((8, 128), F32)
            for r in range(0, size, 8):
                for c in range(0, COLS[u], 128):
                    s = s + t2[r:r + 8, c:c + 128]
            sqv[0] += s
            keep_copy(u, i).start()
            gather_copy(4, u, i).start()

    def h_gather5(i):
        for u in range(2):
            keep_copy(u, i).wait()
            gather_copy(4, u, i).wait()
            gather_copy(5, u, i).start()

    def h_gather(k, i):
        for u in range(2):
            gather_copy(k - 1, u, i).wait()
            gather_copy(k, u, i).start()

    def h_done(i):
        for u in range(2):
            gather_copy(7, u, i).wait()

    plan = {
        0: [(3, functools.partial(h_scatter, 2)), (4, functools.partial(h_scatter, 3))],
        1: [(1, h_pair), (9, h_done), (8, functools.partial(h_gather, 7))],
        2: [(1, h_scatter1)],
        3: [(4, h_final), (5, h_gather5), (6, functools.partial(h_gather, 6))],
    }

    def hooks(g, c):
        for lag, fn in plan[c]:
            i = g - lag

            @pl.when(jnp.logical_and(i >= 0, i < BLOCKS))
            def _():
                fn(i)

    def wcopies(nxt, wf_hbm, wb_hbm):
        at = pl.multiple_of((nxt % STEPS) * BC, BC)
        return (pltpu.make_async_copy(wf_hbm.at[:, pl.ds(at, BC)], wf.at[nxt % 2], wsem.at[0, nxt % 2]),
                pltpu.make_async_copy(wb_hbm.at[pl.ds(at, BC), :], wb.at[nxt % 2], wsem.at[1, nxt % 2]))

    def wload(nxt):
        @pl.when(nxt < STEPS)
        def _():
            for cp in wcopies(nxt, wf0, wb0):
                cp.start()

        @pl.when(jnp.logical_and(nxt >= STEPS, nxt < BLOCKS))
        def _():
            for cp in wcopies(nxt, wf1, wb1):
                cp.start()

    def rows(c):
        return pl.ds(c * MC, MC)

    def dots(c, slot):
        av[c % 2] = nn(pv[rows(c), :], wf[slot]).astype(BF16)
        hv[c % 2] = nt(qv[rows(c), :], wb[slot]).astype(BF16)

    def elem(s):
        for k in range(MC // EC):
            rr = pl.ds(k * EC, EC)
            g, d = gelu_pair(av[s, rr, :], hv[s, rr, :])
            gv[s, rr, :] = g
            dv[s, rr, :] = d

    def grads(c, slot, bslot):
        s = c % 2
        b = tn(gv[s], qv[rows(c), :])
        a = tn(pv[rows(c), :], dv[s])
        if c == 0:
            own_b[bslot] = b
            own_a[bslot] = a
        else:
            own_b[bslot] += b
            own_a[bslot] += a
        acc[rows(c), :] += nt(dv[s], wf[slot])

    bar = pltpu.get_barrier_semaphore()
    for peer in (partner, along(0)[1], along(1)[1], along(2)[1]):
        pl.semaphore_signal(bar, inc=1, device_id=peer, device_id_type=MESH)
    pl.semaphore_wait(bar, 4)

    wload(0)
    pcopy = pltpu.make_async_copy(p0, pv, psem.at[0])
    qcopy = pltpu.make_async_copy(q0, qv, psem.at[1])
    pcopy.start()
    qcopy.start()
    sqv[...] = jnp.zeros(sqv.shape, F32)
    pcopy.wait()
    qcopy.wait()

    def acc_init(k, _):
        rr = pl.ds(pl.multiple_of(k * 128, 128), 128)
        acc[rr, :] = qv[rr, :].astype(F32)
        return 0

    lax.fori_loop(0, TOK // 128, acc_init, 0)

    def phase(ph, _):
        zero = jnp.zeros((MC, BC), BF16)
        av[1] = zero
        hv[1] = zero
        gv[0] = zero
        dv[0] = zero

        def step(j, _):
            g = ph * STEPS + j
            slot = g % 2
            for cp in wcopies(g, wf0, wb0):
                cp.wait()
            for c in range(NCH):
                dots(c, slot)
                elem((c + 1) % 2)
                if c < 2:
                    grads(c + 2, 1 - slot, 1 - slot)
                else:
                    grads(c - 2, slot, slot)
                if c == 1:
                    wload(g + 1)
                hooks(g, c)
            return 0

        lax.fori_loop(0, STEPS, step, 0)
        elem(1)
        grads(2, 1, 1)
        grads(3, 1, 1)

        @pl.when(ph == 0)
        def _():
            cp = pltpu.make_async_copy(p1, pv, psem.at[0])
            cp.start()

            def turn(k, _):
                rr = pl.ds(pl.multiple_of(k * 128, 128), 128)
                q = acc[rr, :].astype(BF16)
                qv[rr, :] = q
                acc[rr, :] = q.astype(F32)
                return 0

            lax.fori_loop(0, TOK // 128, turn, 0)
            cp.wait()

        @pl.when(ph == 1)
        def _():
            def turn(k, _):
                rr = pl.ds(pl.multiple_of(k * 128, 128), 128)
                qv[rr, :] = acc[rr, :].astype(BF16)
                return 0

            lax.fori_loop(0, TOK // 128, turn, 0)
            pltpu.make_async_copy(qv, dx_out, psem.at[1]).start()

        return 0

    lax.fori_loop(0, 2, phase, 0)

    def drain(g, _):
        for c in range(NCH):
            hooks(g, c)
        return 0

    lax.fori_loop(BLOCKS, BLOCKS + 10, drain, 0)

    for k, peer in enumerate((partner, along(0)[1], along(1)[1], along(2)[1])):
        cp = pltpu.make_async_remote_copy(
            src_ref=sqv.at[k], dst_ref=sqr.at[k], send_sem=nsend.at[k], recv_sem=nrecv.at[k],
            device_id=peer, device_id_type=MESH)
        cp.start()
        cp.wait()
        sqv[k + 1] = sqv[k] + sqr[k]
    sq_out[...] = sqv[4]
    pltpu.make_async_copy(qv, dx_out, psem.at[1]).wait()


def run_main(h_two, x_rows, g_rows, w_one, w_two, w_three, w_four):
    vm = pltpu.VMEM
    dma = pltpu.SemaphoreType.DMA
    scratch = [
        vm((TOK, DM), BF16), vm((TOK, DM), BF16), vm((TOK, DM), F32),
        vm((2, DM, BC), BF16), vm((2, BC, DM), BF16),
        vm((2, MC, BC), BF16), vm((2, MC, BC), BF16), vm((2, MC, BC), BF16), vm((2, MC, BC), BF16),
        vm((2, DM, BC), F32), vm((2, BC, DM), F32),
    ]
    for k, slots in ((2, 3), (4, NS), (8, NS), (16, NS)):
        scratch += [vm((slots, ROWS[u] // k, COLS[u]), F32) for u in range(2)]
    scratch += [vm((5, 8, 128), F32), vm((4, 8, 128), F32),
                dma((8, 2, NS)), dma((8, 2, NS)), dma((2, NS)), dma((2, 2)), dma((2,)), dma((4,)), dma((4,))]
    hbm = pl.BlockSpec(memory_space=pl.ANY)
    flops = 2 * 10 * TOK * DM * DF
    return pl.pallas_call(
        main_kernel,
        out_shape=(jax.ShapeDtypeStruct((2, DM, DF), F32), jax.ShapeDtypeStruct((2, DF, DM), F32),
                   jax.ShapeDtypeStruct((TOK, DM), BF16), jax.ShapeDtypeStruct((8, 128), F32)),
        in_specs=[hbm] * 7,
        out_specs=(hbm, hbm, hbm, pl.BlockSpec(memory_space=pltpu.VMEM)),
        scratch_shapes=scratch,
        compiler_params=pltpu.CompilerParams(
            collective_id=0, has_side_effects=True, vmem_limit_bytes=63 * 2 ** 20),
        cost_estimate=pl.CostEstimate(flops=flops, bytes_accessed=200_000_000, transcendentals=2 * TOK * DF),
        name='grad_main',
    )(h_two, x_rows, g_rows, w_three, w_one, w_four, w_two)


def solution(mesh):
    row_spec = P(AXES, None)

    def per_device(x_rows, g_rows, w_one, w_two, w_three, w_four, clip_norm):
        a_one = nn(x_rows, w_one).astype(BF16)
        h_one = jax.nn.gelu(a_one.astype(F32)).astype(BF16)
        h_two = (nn(h_one, w_two) + x_rows.astype(F32)).astype(BF16)
        ta, tb, dx_rows, sq = run_main(h_two, x_rows, g_rows, w_one, w_two, w_three, w_four)
        scale = jnp.minimum(1.0, clip_norm[0] / jnp.sqrt(jnp.sum(sq)))
        return tuple(part * (1.0 / 16) * scale for part in (ta[1], tb[1], ta[0], tb[0])) + (dx_rows,)

    return jax.shard_map(per_device, mesh=mesh, in_specs=(row_spec, row_spec, P(), P(), P(), P(), P()),
                         out_specs=(P(), P(), P(), P(), row_spec), check_vma=False)
```

```python
import functools
import math

import jax
import jax.numpy as jnp
from jax import lax
from jax.experimental import pallas as pl
from jax.experimental.pallas import tpu as pltpu
from jax.sharding import PartitionSpec as P


F32 = jnp.float32
BF16 = jnp.bfloat16
MESH = pl.DeviceIdType.MESH
AXES = ('dz', 'dy', 'dx')
ROOT = math.sqrt(2 / math.pi)
CUBE = ROOT * 0.044715

TOK = 4096
DM = 1024
DF = 4096
BC = 256
STEPS = DF // BC
BLOCKS = 2 * STEPS
MC = 512
PER = 4
EC = 32
NS = 6
LATE = 6
EARLY = BLOCKS - LATE
TAIL = 9


def nn(a, b):
    return jnp.dot(a, b, preferred_element_type=F32)


def nt(a, b):
    return lax.dot_general(a, b, (((1,), (1,)), ((), ())), preferred_element_type=F32)


def tn(a, b):
    return lax.dot_general(a, b, (((0,), (0,)), ((), ())), preferred_element_type=F32)


def gelu_half(pre):
    x = pre.astype(F32)
    sq = x * x
    h = 0.5 * jnp.tanh(x * (ROOT + CUBE * sq)) + 0.5
    return x * h, h, sq


def gelu_pair(pre, up):
    g, h, sq = gelu_half(pre)
    slope = h + g * (1.0 - h) * (2 * ROOT + 6 * CUBE * sq)
    return g.astype(BF16), (up.astype(F32) * slope).astype(BF16)


def main_kernel(x0, g0, wf0, wf1, wb0, wb1,
                ta, tb, late_out, dx_out, sq_out, a_all,
                pv, qv, acc, wf, wb, av, hv, gv, dv, sa,
                own, r0, r1, r2, r3, tv, sqv, sqr,
                ssem, rsem, lsem, wsem, psem, asem, nsend, nrecv):
    zb = lax.axis_index('dz')
    yb = lax.axis_index('dy')
    dxi = lax.axis_index('dx')
    xb = dxi // 2
    cb = dxi % 2
    partner = (zb, yb, 2 * xb + (1 - cb))

    flips = (1 - xb, 1 - yb, 1 - zb)

    def pick(d, x, y, z):
        return jnp.where(d == 0, x, jnp.where(d == 1, y, z))

    def peer_on(d):
        px = jnp.where(d == 0, flips[0], xb)
        return (jnp.where(d == 2, flips[2], zb), jnp.where(d == 1, flips[1], yb), 2 * px + cb)

    def wrap(x, n):
        return jnp.where(x >= n, x - n, x)

    def way(s3, k):
        return wrap(s3 + wrap(cb + k, 3), 3)

    def bit_on(d):
        return pick(d, xb, yb, zb)

    def remote(src, dst, stage, s6, peer):
        return pltpu.make_async_remote_copy(
            src_ref=src, dst_ref=dst, send_sem=ssem.at[stage, s6], recv_sem=rsem.at[stage, s6],
            device_id=peer, device_id_type=MESH)

    def finish(stage, s6):
        ref = (r0, r1, r2, r3, r3, r2, r1, r0)[stage].at[0]
        cp = remote(ref, ref, stage, s6, partner)
        cp.wait_send()
        cp.wait_recv()

    def region(i, core, start, size):
        at = pl.multiple_of((i & (STEPS - 1)) * BC, BC)
        cut = pl.ds(pl.multiple_of(start, 128), size)
        if core == 0:
            return ta.at[i // STEPS, cut, pl.ds(at, BC)]
        return tb.at[i // STEPS, pl.ds(at, BC), cut]

    def both(fn):
        for core in range(2):
            @pl.when(cb == core)
            def _():
                fn(core)

    def side(core):
        return pl.ds(pl.multiple_of(core * BC, BC), BC)

    def cut_of(bit, k):
        size = DM >> k
        return pl.ds(pl.multiple_of(bit * size, 128), size)

    def send_part(k, s6, s3):
        d = way(s3, k - 1)
        bit = bit_on(d)
        src = (r0.at[s3], r1.at[s6], r2.at[s6])[k - 1]
        dst = (r1, r2, r3)[k - 1].at[s6]
        remote(src.at[cut_of(1 - bit, k)], dst, k, s6, peer_on(d)).start()

    def kept(k, s6, s3):
        cut = cut_of(bit_on(way(s3, k - 1)), k)
        if k == 1:
            return r0[s3, cut, :]
        return (r1, r2)[k - 2][s6, cut, :]

    def late_copy(i, s6):
        n = i - EARLY
        return pltpu.make_async_copy(r3.at[s6], late_out.at[n % 3, n // 3], lsem.at[s6])

    def keep_wait(s6):
        pltpu.make_async_copy(r3.at[0], r3.at[0], lsem.at[s6]).wait()

    def h_pair(i, s6, s3):
        remote(own.at[i & 1, :, side(1 - cb)], r0.at[s3], 0, s6, partner).start()

    def h_scatter1(i, s6, s3):
        finish(0, s6)
        r0[s3] += own[i & 1, :, side(cb)]
        send_part(1, s6, s3)

    def h_scatter(k, i, s6, s3):
        finish(k - 1, s6)
        (r1, r2)[k - 2][s6] += kept(k - 1, s6, s3)
        send_part(k, s6, s3)

    def h_final(i, s6, s3):
        finish(3, s6)
        tot = r3[s6] + kept(3, s6, s3)
        t2 = jnp.square(tot * (1.0 / 16))
        s = jnp.zeros((8, 128), F32)
        for r in range(0, DM // 8, 8):
            for c in range(0, BC, 128):
                s = s + t2[r:r + 8, c:c + 128]
        sqv[0] += s

        @pl.when(i >= EARLY)
        def _():
            r3[s6] = tot
            late_copy(i, s6).start()

        def put(core):
            if core == 0:
                r3[s6] = tot
            else:
                tv[i & 1] = tot.T
            src = r3.at[s6] if core == 0 else tv.at[i & 1]
            d = [way(s3, k) for k in range(3)]
            start = bit_on(d[0]) * (DM // 2) + bit_on(d[1]) * (DM // 4) + bit_on(d[2]) * (DM // 8)
            dst = region(i, core, start, DM // 8)
            pltpu.make_async_copy(src, dst, lsem.at[s6]).start()
            remote(src, dst, 4, s6, peer_on(d[2])).start()

        @pl.when(i < EARLY)
        def _():
            both(put)

    def h_gather(k, i, s6, s3):
        def move(core):
            if k == 7:
                part = region(i, core, 0, DM)
                remote(part, part, k, s6, partner).start()
            else:
                d = [way(s3, j) for j in range(7 - k)]
                start = bit_on(d[0]) * (DM // 2)
                if k == 5:
                    start = start + bit_on(d[1]) * (DM // 4)
                part = region(i, core, start, DM >> (7 - k))
                remote(part, part, k, s6, peer_on(d[-1])).start()

        if k == 5:
            keep_wait(s6)

        @pl.when(i < EARLY)
        def _():
            finish(k - 1, s6)
            both(move)

    def h_done(i, s6, s3):
        finish(7, s6)

    plan = [(18, h_done), (16, functools.partial(h_gather, 7)), (10, functools.partial(h_gather, 6)),
            (8, functools.partial(h_gather, 5)), (7, h_final), (6, functools.partial(h_scatter, 3)),
            (4, functools.partial(h_scatter, 2)), (1, h_scatter1), (0, h_pair)]

    def hooks(n):
        g = n // 2
        g6 = g % NS
        for lag, fn in plan:
            back = 1 + lag // 2
            i = g - back
            top = EARLY if lag > 8 else BLOCKS

            @pl.when(jnp.logical_and((n & 1) == lag % 2, jnp.logical_and(i >= 0, i < top)))
            def _():
                s6 = wrap(g6 + NS - back % NS, NS)
                fn(i, s6, wrap(s6, 3))

    def wcopies(g, wf_hbm, wb_hbm):
        at = pl.multiple_of((g % STEPS) * BC, BC)
        return (pltpu.make_async_copy(wf_hbm.at[:, pl.ds(at, BC)], wf.at[g % 3], wsem.at[0, g % 3]),
                pltpu.make_async_copy(wb_hbm.at[pl.ds(at, BC), :], wb.at[g % 3], wsem.at[1, g % 3]))

    def wload(g):
        mid = jnp.logical_and(g >= STEPS, g < 2 * STEPS)

        @pl.when(mid)
        def _():
            for cp in wcopies(g, wf0, wb0):
                cp.start()

        @pl.when(jnp.logical_and(jnp.logical_not(mid), g < 3 * STEPS))
        def _():
            for cp in wcopies(g, wf1, wb1):
                cp.start()

    def wnext(g):
        wload(g + 2)

        @pl.when(g + 1 < 3 * STEPS)
        def _():
            for cp in wcopies(g + 1, wf0, wb0):
                cp.wait()

    def rows(c):
        return pl.ds(pl.multiple_of(c * MC, MC), MC)

    def back_rows(h, u, k):
        return rows(PER * h + u - k if u >= k else PER * (1 - h) + PER + u - k)

    def a_store(g):
        return pltpu.make_async_copy(sa.at[g % 2], a_all.at[g], asem.at[g % 2])

    def a_load(j):
        return pltpu.make_async_copy(a_all.at[j], sa.at[j % 2], asem.at[j % 2])

    def elem(s, a_ref, at):
        for k in range(MC // EC):
            rr = pl.ds(k * EC, EC)
            ar = rr if at is None else pl.ds(pl.multiple_of(at * MC + k * EC, EC), EC)
            g, d = gelu_pair(a_ref[ar, :], hv[s, rr, :])
            gv[s, rr, :] = g
            dv[s, rr, :] = d

    def felem(s):
        for k in range(MC // EC):
            rr = pl.ds(k * EC, EC)
            gv[s, rr, :] = gelu_half(av[s, rr, :])[0].astype(BF16)

    def add_acc(rr, first, term):
        acc[rr, :] = jnp.where(first, qv[rr, :].astype(F32), acc[rr, :]) + term

    def fgrads(s, rr, gp):
        add_acc(rr, gp == 0, nn(gv[s], wb[(gp + 3) % 3]))

    def grads(s, rr, j, i, fresh):
        a = tn(pv[rr, :], dv[s])
        b = tn(qv[rr, :], gv[s])
        slot = (i + 2) % 2
        if fresh is not None:
            own[slot, :, :BC] = a + jnp.where(fresh, 0.0, own[slot, :, :BC])
            own[slot, :, BC:] = b + jnp.where(fresh, 0.0, own[slot, :, BC:])
        else:
            own[slot, :, :BC] += a
            own[slot, :, BC:] += b
        add_acc(rr, j == 0, nt(dv[s], wf[(i + STEPS) % 3]))

    def sweep(fn):
        def body(k, _):
            fn(pl.ds(pl.multiple_of(k * 256, 256), 256))
            return 0

        lax.fori_loop(0, TOK // 256, body, 0)

    zero = jnp.zeros((MC, BC), BF16)

    bar = pltpu.get_barrier_semaphore()
    for peer in (partner, peer_on(0), peer_on(1), peer_on(2)):
        pl.semaphore_signal(bar, inc=1, device_id=peer, device_id_type=MESH)
    pl.semaphore_wait(bar, 4)

    wload(0)
    wload(1)
    xcopy = pltpu.make_async_copy(x0, qv, psem.at[1])
    xcopy.start()
    sqv[...] = jnp.zeros(sqv.shape, F32)
    av[1] = zero
    gv[0] = zero
    xcopy.wait()
    for cp in wcopies(0, wf0, wb0):
        cp.wait()

    def fhalf(q, _):
        g = q // 2
        h = q & 1
        for u in range(PER):
            rr = rows(PER * h + u)
            a = nn(qv[rr, :], wf[g % 3]).astype(BF16)
            av[u % 2] = a
            sa[g & 1, rr, :] = a
            felem(1 - u % 2)
            fgrads(u % 2, back_rows(h, u, 2), g - 1 + h if u < 2 else g)

        @pl.when(h == 1)
        def _():
            wnext(g)
            a_store(g).start()

            @pl.when(g > 0)
            def _():
                a_store(g - 1).wait()

        return 0

    lax.fori_loop(0, 2 * STEPS, fhalf, 0)
    felem(1)
    fgrads(0, rows(2 * PER - 2), STEPS - 1)
    fgrads(1, rows(2 * PER - 1), STEPS - 1)
    gcopy = pltpu.make_async_copy(g0, qv, psem.at[1])
    gcopy.start()

    def h_two(rr):
        pv[rr, :] = acc[rr, :].astype(BF16)

    sweep(h_two)
    a_store(STEPS - 1).wait()
    gcopy.wait()

    def half(ph, q):
        j = q // 2
        h = q & 1
        g = ph * STEPS + j
        for u in range(PER):
            v = u % 2
            rr = rows(PER * h + u)
            if ph == 0:
                av[v] = nn(pv[rr, :], wf[(g + STEPS) % 3]).astype(BF16)
            hv[v] = nt(qv[rr, :], wb[(g + STEPS) % 3]).astype(BF16)
            if ph == 0:
                elem(1 - v, av.at[1 - v], None)
            elif u == 0:
                elem(1 - v, sa.at[(j + 1 + h) & 1], PER * (1 - h) + PER - 1)
            else:
                elem(1 - v, sa.at[j & 1], PER * h + u - 1)
            back = 1 - h if u < 2 else 0
            grads(v, back_rows(h, u, 2), j - back, g - back, h == 0 if u == 2 else None)

        @pl.when(h == 1)
        def _():
            wnext(g + STEPS)

        if ph == 1:
            @pl.when(j + 1 < STEPS)
            def _():
                @pl.when(h == 0)
                def _():
                    a_load(j + 1).start()

                @pl.when(h == 1)
                def _():
                    a_load(j + 1).wait()

        hooks(2 * g + h)

    def turn(rr):
        qv[rr, :] = acc[rr, :].astype(BF16)

    for ph in range(2):
        hv[1] = zero
        gv[0] = zero
        dv[0] = zero
        if ph == 0:
            av[1] = zero
        lax.fori_loop(0, 2 * STEPS, lambda q, _, ph=ph: (half(ph, q), 0)[1], 0)
        last = ph * STEPS + STEPS - 1
        if ph == 0:
            a_load(0).start()
            sa[1, TOK - MC:, :] = zero
            elem(1, av.at[1], None)
        else:
            elem(1, sa.at[1], 2 * PER - 1)
        grads(0, rows(2 * PER - 2), STEPS - 1, last, None)
        grads(1, rows(2 * PER - 1), STEPS - 1, last, None)
        if ph == 0:
            pcopy = pltpu.make_async_copy(x0, pv, psem.at[0])
            pcopy.start()
            sweep(turn)
            pcopy.wait()
            a_load(0).wait()
        else:
            sweep(turn)
            pltpu.make_async_copy(qv, dx_out, psem.at[1]).start()

    def drain(n, _):
        hooks(n)
        return 0

    lax.fori_loop(2 * BLOCKS, 2 * BLOCKS + TAIL, drain, 0)

    for k, peer in enumerate((partner, peer_on(0), peer_on(1), peer_on(2))):
        cp = pltpu.make_async_remote_copy(
            src_ref=sqv.at[k], dst_ref=sqr.at[k], send_sem=nsend.at[k], recv_sem=nrecv.at[k],
            device_id=peer, device_id_type=MESH)
        cp.start()
        cp.wait()
        sqv[k + 1] = sqv[k] + sqr[k]
    sq_out[...] = sqv[4]
    pltpu.make_async_copy(qv, dx_out, psem.at[1]).wait()


def run_main(x_rows, g_rows, w_one, w_two, w_three, w_four):
    vm = pltpu.VMEM
    dma = pltpu.SemaphoreType.DMA
    out = jax.ShapeDtypeStruct
    scratch = [
        vm((TOK, DM), BF16), vm((TOK, DM), BF16), vm((TOK, DM), F32),
        vm((3, DM, BC), BF16), vm((3, BC, DM), BF16),
        vm((2, MC, BC), BF16), vm((2, MC, BC), BF16), vm((2, MC, BC), BF16), vm((2, MC, BC), BF16),
        vm((2, TOK, BC), BF16),
        vm((2, DM, 2 * BC), F32), vm((3, DM, BC), F32), vm((NS, DM // 2, BC), F32),
        vm((NS, DM // 4, BC), F32), vm((NS, DM // 8, BC), F32), vm((2, BC, DM // 8), F32),
        vm((5, 8, 128), F32), vm((4, 8, 128), F32),
        dma((8, NS)), dma((8, NS)), dma((NS,)), dma((2, 3)), dma((2,)), dma((2,)), dma((4,)), dma((4,)),
    ]
    hbm = pl.BlockSpec(memory_space=pl.ANY)
    return pl.pallas_call(
        main_kernel,
        out_shape=(out((2, DM, DF), F32), out((2, DF, DM), F32), out((3, LATE // 3, DM // 8, BC), F32),
                   out((TOK, DM), BF16), out((8, 128), F32), out((STEPS, TOK, BC), BF16)),
        in_specs=[hbm] * 6,
        out_specs=(hbm, hbm, hbm, hbm, pl.BlockSpec(memory_space=pltpu.VMEM), hbm),
        scratch_shapes=scratch,
        compiler_params=pltpu.CompilerParams(
            collective_id=0, has_side_effects=True, vmem_limit_bytes=63 * 2 ** 20),
        cost_estimate=pl.CostEstimate(flops=2 * 11 * TOK * DM * DF, bytes_accessed=250_000_000,
                                      transcendentals=3 * TOK * DF),
        name='grad_main',
    )(x_rows, g_rows, w_three, w_one, w_four, w_two)


def scaled(x, scale):
    return x * (1.0 / 16) * scale


def early_kernel(scale, ta_ref, tb_ref, oa_ref, ob_ref):
    oa_ref[...] = scaled(ta_ref[0], scale[0])
    ob_ref[...] = scaled(tb_ref[0], scale[0])


def write_early(ta, tb, scale, ph, steps):
    n = 8
    wide = steps * BC
    return pl.pallas_call(
        early_kernel,
        out_shape=(jax.ShapeDtypeStruct((DM, DF), F32), jax.ShapeDtypeStruct((DF, DM), F32)),
        grid=(n,),
        in_specs=[pl.BlockSpec(memory_space=pltpu.SMEM),
                  pl.BlockSpec((1, DM // n, wide), lambda j: (ph, j, 0)),
                  pl.BlockSpec((1, wide // n, DM), lambda j: (ph, j, 0))],
        out_specs=(pl.BlockSpec((DM // n, wide), lambda j: (j, 0)), pl.BlockSpec((wide // n, DM), lambda j: (j, 0))),
        cost_estimate=pl.CostEstimate(flops=50_000_000 * steps, bytes_accessed=16 * DM * BC * steps,
                                      transcendentals=0),
        name='write_early',
    )(scale, ta, tb)


def copy_kernel(src, dst):
    dst[...] = src[...]


def copy_rows(x):
    spec = pl.BlockSpec((TOK // 4, DM), lambda j: (j, 0))
    return pl.pallas_call(
        copy_kernel, out_shape=jax.ShapeDtypeStruct(x.shape, x.dtype), grid=(4,), in_specs=[spec], out_specs=spec,
        cost_estimate=pl.CostEstimate(flops=20_000_000, bytes_accessed=4 * TOK * DM, transcendentals=0),
        name='copy_rows',
    )(x)


def late_kernel(far, scale, m0, m1, m2, o0, o1, o2, oa_in, ob_in, oa, ob, buf_a, buf_b, sem):
    dxi = lax.axis_index('dx')
    core = dxi % 2
    bits = (dxi // 2, lax.axis_index('dy'), lax.axis_index('dz'))
    copies = []
    for group, (mine, other) in enumerate(((m0, o0), (m1, o1), (m2, o2))):
        place = [[bits[(EARLY + group + c + k) % 3] for k in range(3)] for c in range(2)]
        for m in range(LATE // 3):
            col = (EARLY % STEPS + group + 3 * m) * BC
            for h in range(2):
                n = len(copies) // 2
                for f in range(2):
                    x = mine[h, f, m]
                    y = other[h, f, m]
                    a = jnp.where(core == 0, x, y)
                    b = jnp.where(core == 0, y, x)
                    at_a = pl.multiple_of((f + place[0][2]) % 2 * 128, 128)
                    at_b = pl.multiple_of((f + place[1][2]) % 2 * 128, 128)
                    buf_a[n, pl.ds(at_a, 128), :] = scaled(a, scale[0])
                    buf_b[n, :, pl.ds(at_b, 128)] = scaled(b, scale[0]).T
                ra, rb = ((place[c][0] + far) % 2 * 512 + (place[c][1] + h) % 2 * 256 for c in range(2))
                copies.append(pltpu.make_async_copy(
                    buf_a.at[n], oa.at[pl.ds(pl.multiple_of(ra, 256), 256), pl.ds(col, BC)], sem.at[0, n]))
                copies.append(pltpu.make_async_copy(
                    buf_b.at[n], ob.at[pl.ds(col, BC), pl.ds(pl.multiple_of(rb, 256), 256)], sem.at[1, n]))
                copies[-2].start()
                copies[-1].start()
    for cp in copies:
        cp.wait()


def write_late(scale, mine, other, out_a, out_b, far):
    n = 2 * LATE
    vmem = pl.BlockSpec(memory_space=pltpu.VMEM)
    hbm = pl.BlockSpec(memory_space=pl.ANY)
    return pl.pallas_call(
        functools.partial(late_kernel, far),
        out_shape=(jax.ShapeDtypeStruct((DM, DF), F32), jax.ShapeDtypeStruct((DF, DM), F32)),
        in_specs=[pl.BlockSpec(memory_space=pltpu.SMEM)] + [vmem] * 6 + [hbm] * 2,
        out_specs=(hbm, hbm),
        scratch_shapes=[pltpu.VMEM((n, DM // 4, BC), F32), pltpu.VMEM((n, BC, DM // 4), F32),
                        pltpu.SemaphoreType.DMA((2, n))],
        input_output_aliases={7: 0, 8: 1},
        cost_estimate=pl.CostEstimate(flops=60_000_000, bytes_accessed=8 * DM * BC * LATE, transcendentals=0),
        name='write_late',
    )(scale, *mine, *other, out_a, out_b)


def solution(mesh):
    row_spec = P(AXES, None)
    masks = (2, 4, 8)

    def hop(x, group, k):
        first = (EARLY + group) % 3
        pairs = [(r, r ^ masks[(first + r % 2 + k) % 3]) for r in range(16)]
        return lax.ppermute(x, AXES, pairs)

    def per_device(x_rows, g_rows, w_one, w_two, w_three, w_four, clip_norm):
        ta, tb, late, dx_rows, sq, _ = run_main(x_rows, g_rows, w_one, w_two, w_three, w_four)
        scale = jnp.minimum(1.0, clip_norm / jnp.sqrt(jnp.sum(sq)))
        swap = [(r, r ^ 1) for r in range(16)]
        groups = range(3)
        got = [hop(late[n], n, 2) for n in groups]
        dx_rows = copy_rows(dx_rows)
        got, dx_rows = lax.optimization_barrier((got, dx_rows))
        pair = [jnp.stack([late[n], got[n]]) for n in groups]
        got = [hop(pair[n], n, 1) for n in groups]
        g_one, g_two = write_early(ta, tb, scale, 1, EARLY - STEPS)
        got, g_one, g_two = lax.optimization_barrier((got, g_one, g_two))
        near = [jnp.stack([pair[n], got[n]]) for n in groups]
        far = [hop(near[n], n, 0) for n in groups]
        other = [lax.ppermute(near[n], AXES, swap) for n in groups]
        g_three, g_four = write_early(ta, tb, scale, 0, STEPS)
        other, g_three, g_four = lax.optimization_barrier((other, g_three, g_four))
        g_one, g_two = write_late(scale, near, other, g_one, g_two, 0)
        far, g_one, g_two = lax.optimization_barrier((far, g_one, g_two))
        other = [lax.ppermute(far[n], AXES, swap) for n in groups]
        g_one, g_two = write_late(scale, far, other, g_one, g_two, 1)
        return g_one, g_two, g_three, g_four, dx_rows

    return jax.shard_map(per_device, mesh=mesh, in_specs=(row_spec, row_spec, P(), P(), P(), P(), P()),
                         out_specs=(P(), P(), P(), P(), row_spec), check_vma=False)
```

```python
import functools
import math

import jax
import jax.numpy as jnp
from jax import lax
from jax.experimental import pallas as pl
from jax.experimental.pallas import tpu as pltpu
from jax.sharding import PartitionSpec as P


F32 = jnp.float32
BF16 = jnp.bfloat16
MESH = pl.DeviceIdType.MESH
AXES = ('dz', 'dy', 'dx')
ROOT = math.sqrt(2 / math.pi)
CUBE = ROOT * 0.044715

TOK = 4096
DM = 1024
DF = 4096
BC = 256
STEPS = DF // BC
BLOCKS = 2 * STEPS
MC = 512
PER = 4
EC = 32
NS = 6
LATE = 9
EARLY = BLOCKS - LATE
TAIL = 13


def nn(a, b):
    return jnp.dot(a, b, preferred_element_type=F32)


def nt(a, b):
    return lax.dot_general(a, b, (((1,), (1,)), ((), ())), preferred_element_type=F32)


def tn(a, b):
    return lax.dot_general(a, b, (((0,), (0,)), ((), ())), preferred_element_type=F32)


def gelu_half(pre):
    x = pre.astype(F32)
    sq = x * x
    h = 0.5 * jnp.tanh(x * (ROOT + CUBE * sq)) + 0.5
    return x * h, h, sq


def gelu_pair(pre, up):
    g, h, sq = gelu_half(pre)
    slope = h + g * (1.0 - h) * (2 * ROOT + 6 * CUBE * sq)
    return g.astype(BF16), (up.astype(F32) * slope).astype(BF16)


def main_kernel(x0, g0, wf0, wf1, wb0, wb1,
                ta, tb, late0, late1, late2, dx_out, sq_out, a_all,
                pv, qv, acc, wf, wb, av, hv, gv, dv, sa,
                own, r0, r1, r2, r3, tv, sqv, sqr,
                ssem, rsem, lsem, wsem, psem, asem, nsend, nrecv):
    zb = lax.axis_index('dz')
    yb = lax.axis_index('dy')
    dxi = lax.axis_index('dx')
    xb = dxi // 2
    cb = dxi % 2
    partner = (zb, yb, 2 * xb + (1 - cb))

    flips = (1 - xb, 1 - yb, 1 - zb)

    def pick(d, x, y, z):
        return jnp.where(d == 0, x, jnp.where(d == 1, y, z))

    def peer_on(d):
        px = jnp.where(d == 0, flips[0], xb)
        return (jnp.where(d == 2, flips[2], zb), jnp.where(d == 1, flips[1], yb), 2 * px + cb)

    def wrap(x, n):
        return jnp.where(x >= n, x - n, x)

    def way(s3, k):
        return wrap(s3 + wrap(cb + k, 3), 3)

    def bit_on(d):
        return pick(d, xb, yb, zb)

    def remote(src, dst, stage, s6, peer):
        return pltpu.make_async_remote_copy(
            src_ref=src, dst_ref=dst, send_sem=ssem.at[stage, s6], recv_sem=rsem.at[stage, s6],
            device_id=peer, device_id_type=MESH)

    def finish(stage, s6):
        ref = (r0, r1, r2, r3, r3, r2, r1, r0)[stage].at[0]
        cp = remote(ref, ref, stage, s6, partner)
        cp.wait_send()
        cp.wait_recv()

    def region(i, core, start, size):
        at = pl.multiple_of((i & (STEPS - 1)) * BC, BC)
        cut = pl.ds(pl.multiple_of(start, 128), size)
        if core == 0:
            return ta.at[i // STEPS, cut, pl.ds(at, BC)]
        return tb.at[i // STEPS, pl.ds(at, BC), cut]

    def both(fn):
        for core in range(2):
            @pl.when(cb == core)
            def _():
                fn(core)

    def side(core):
        return pl.ds(pl.multiple_of(core * BC, BC), BC)

    def cut_of(bit, k):
        size = DM >> k
        return pl.ds(pl.multiple_of(bit * size, 128), size)

    def send_part(k, s6, s3):
        d = way(s3, k - 1)
        bit = bit_on(d)
        src = (r0.at[s3], r1.at[s6], r2.at[s6])[k - 1]
        dst = (r1, r2, r3)[k - 1].at[s6]
        remote(src.at[cut_of(1 - bit, k)], dst, k, s6, peer_on(d)).start()

    def kept(k, s6, s3):
        cut = cut_of(bit_on(way(s3, k - 1)), k)
        if k == 1:
            return r0[s3, cut, :]
        return (r1, r2)[k - 2][s6, cut, :]

    def late_copy(i, s6):
        n = i - EARLY
        for group, out in enumerate((late0, late1, late2)):
            @pl.when(n % 3 == group)
            def _():
                pltpu.make_async_copy(r3.at[s6], out.at[n // 3], lsem.at[s6]).start()

    def keep_wait(s6):
        pltpu.make_async_copy(r3.at[0], r3.at[0], lsem.at[s6]).wait()

    def h_pair(i, s6, s3):
        remote(own.at[i & 1, :, side(1 - cb)], r0.at[s3], 0, s6, partner).start()

    def h_scatter1(i, s6, s3):
        finish(0, s6)
        r0[s3] += own[i & 1, :, side(cb)]
        send_part(1, s6, s3)

    def h_scatter(k, i, s6, s3):
        finish(k - 1, s6)
        (r1, r2)[k - 2][s6] += kept(k - 1, s6, s3)
        send_part(k, s6, s3)

    def h_final(i, s6, s3):
        finish(3, s6)
        tot = r3[s6] + kept(3, s6, s3)
        t2 = jnp.square(tot * (1.0 / 16))
        s = jnp.zeros((8, 128), F32)
        for r in range(0, DM // 8, 8):
            for c in range(0, BC, 128):
                s = s + t2[r:r + 8, c:c + 128]
        sqv[0] += s

        @pl.when(i >= EARLY)
        def _():
            r3[s6] = tot
            late_copy(i, s6)

        def put(core):
            if core == 0:
                r3[s6] = tot
            else:
                tv[i & 1] = tot.T
            src = r3.at[s6] if core == 0 else tv.at[i & 1]
            d = [way(s3, k) for k in range(3)]
            start = bit_on(d[0]) * (DM // 2) + bit_on(d[1]) * (DM // 4) + bit_on(d[2]) * (DM // 8)
            dst = region(i, core, start, DM // 8)
            pltpu.make_async_copy(src, dst, lsem.at[s6]).start()
            remote(src, dst, 4, s6, peer_on(d[2])).start()

        @pl.when(i < EARLY)
        def _():
            both(put)

    def h_gather(k, i, s6, s3):
        def move(core):
            if k == 7:
                part = region(i, core, 0, DM)
                remote(part, part, k, s6, partner).start()
            else:
                d = [way(s3, j) for j in range(7 - k)]
                start = bit_on(d[0]) * (DM // 2)
                if k == 5:
                    start = start + bit_on(d[1]) * (DM // 4)
                part = region(i, core, start, DM >> (7 - k))
                remote(part, part, k, s6, peer_on(d[-1])).start()

        if k == 5:
            keep_wait(s6)

        @pl.when(i < EARLY)
        def _():
            finish(k - 1, s6)
            both(move)

    def h_done(i, s6, s3):
        finish(7, s6)

    plan = [(28, h_done), (22, functools.partial(h_gather, 7)), (16, functools.partial(h_gather, 6)),
            (12, functools.partial(h_gather, 5)), (10, h_final), (7, functools.partial(h_scatter, 3)),
            (4, functools.partial(h_scatter, 2)), (1, h_scatter1), (0, h_pair)]

    def hooks(n):
        g = n // 2
        g6 = g % NS
        for lag, fn in plan:
            back = 1 + lag // 2
            i = g - back
            top = EARLY if lag > 12 else BLOCKS

            @pl.when(jnp.logical_and((n & 1) == lag % 2, jnp.logical_and(i >= 0, i < top)))
            def _():
                s6 = wrap(g6 + NS - back % NS, NS)
                fn(i, s6, wrap(s6, 3))

    def wcopies(g, wf_hbm, wb_hbm):
        at = pl.multiple_of((g % STEPS) * BC, BC)
        return (pltpu.make_async_copy(wf_hbm.at[:, pl.ds(at, BC)], wf.at[g % 3], wsem.at[0, g % 3]),
                pltpu.make_async_copy(wb_hbm.at[pl.ds(at, BC), :], wb.at[g % 3], wsem.at[1, g % 3]))

    def wload(g):
        mid = jnp.logical_and(g >= STEPS, g < 2 * STEPS)

        @pl.when(mid)
        def _():
            for cp in wcopies(g, wf0, wb0):
                cp.start()

        @pl.when(jnp.logical_and(jnp.logical_not(mid), g < 3 * STEPS))
        def _():
            for cp in wcopies(g, wf1, wb1):
                cp.start()

    def wnext(g):
        wload(g + 2)

        @pl.when(g + 1 < 3 * STEPS)
        def _():
            for cp in wcopies(g + 1, wf0, wb0):
                cp.wait()

    def rows(c):
        return pl.ds(pl.multiple_of(c * MC, MC), MC)

    def back_rows(h, u, k):
        return rows(PER * h + u - k if u >= k else PER * (1 - h) + PER + u - k)

    def a_store(g):
        return pltpu.make_async_copy(sa.at[g % 2], a_all.at[g], asem.at[g % 2])

    def a_load(j):
        return pltpu.make_async_copy(a_all.at[j], sa.at[j % 2], asem.at[j % 2])

    def elem(s, a_ref, at):
        for k in range(MC // EC):
            rr = pl.ds(k * EC, EC)
            ar = rr if at is None else pl.ds(pl.multiple_of(at * MC + k * EC, EC), EC)
            g, d = gelu_pair(a_ref[ar, :], hv[s, rr, :])
            gv[s, rr, :] = g
            dv[s, rr, :] = d

    def felem(s):
        for k in range(MC // EC):
            rr = pl.ds(k * EC, EC)
            gv[s, rr, :] = gelu_half(av[s, rr, :])[0].astype(BF16)

    def add_acc(rr, first, start, term):
        acc[rr, :] = jnp.where(first, start[rr, :].astype(F32), acc[rr, :]) + term

    def fgrads(s, rr, gp):
        add_acc(rr, gp == 0, pv, nn(gv[s], wb[(gp + 3) % 3]))

    def grads(s, rr, j, i, fresh):
        a = tn(pv[rr, :], dv[s])
        b = tn(qv[rr, :], gv[s])
        slot = (i + 2) % 2
        if fresh is not None:
            own[slot, :, :BC] = a + jnp.where(fresh, 0.0, own[slot, :, :BC])
            own[slot, :, BC:] = b + jnp.where(fresh, 0.0, own[slot, :, BC:])
        else:
            own[slot, :, :BC] += a
            own[slot, :, BC:] += b
        add_acc(rr, j == 0, qv, nt(dv[s], wf[(i + STEPS) % 3]))

    def sweep(fn):
        def body(k, _):
            fn(pl.ds(pl.multiple_of(k * 256, 256), 256))
            return 0

        lax.fori_loop(0, TOK // 256, body, 0)

    zero = jnp.zeros((MC, BC), BF16)

    bar = pltpu.get_barrier_semaphore()
    row = [(zb, yb, 2 * (1 - xb) + 1 - cb), peer_on(0), partner]
    plane = [(1 - zb, 1 - yb, dxi), peer_on(1), peer_on(2)]
    for peer in row + plane:
        pl.semaphore_signal(bar, inc=1, device_id=peer, device_id_type=MESH)
    pl.semaphore_wait(bar, 6)

    wload(0)
    wload(1)
    xcopy = pltpu.make_async_copy(x0, pv, psem.at[0])
    xcopy.start()
    gcopy = pltpu.make_async_copy(g0, qv, psem.at[1])
    gcopy.start()
    sqv[...] = jnp.zeros(sqv.shape, F32)
    av[1] = zero
    gv[0] = zero
    xcopy.wait()
    for cp in wcopies(0, wf0, wb0):
        cp.wait()

    def fhalf(q, _):
        g = q // 2
        h = q & 1
        for u in range(PER):
            rr = rows(PER * h + u)
            a = nn(pv[rr, :], wf[g % 3]).astype(BF16)
            av[u % 2] = a
            sa[g & 1, rr, :] = a
            felem(1 - u % 2)
            fgrads(u % 2, back_rows(h, u, 2), g - 1 + h if u < 2 else g)

        @pl.when(h == 1)
        def _():
            wnext(g)
            a_store(g).start()

            @pl.when(g > 0)
            def _():
                a_store(g - 1).wait()

        return 0

    lax.fori_loop(0, 2 * STEPS, fhalf, 0)
    felem(1)
    fgrads(0, rows(2 * PER - 2), STEPS - 1)
    fgrads(1, rows(2 * PER - 1), STEPS - 1)

    def h_two(rr):
        pv[rr, :] = acc[rr, :].astype(BF16)

    sweep(h_two)
    a_store(STEPS - 1).wait()
    gcopy.wait()

    def half(ph, q):
        j = q // 2
        h = q & 1
        g = ph * STEPS + j
        for u in range(PER):
            v = u % 2
            rr = rows(PER * h + u)
            if ph == 0:
                av[v] = nn(pv[rr, :], wf[(g + STEPS) % 3]).astype(BF16)
            hv[v] = nt(qv[rr, :], wb[(g + STEPS) % 3]).astype(BF16)
            if ph == 0:
                elem(1 - v, av.at[1 - v], None)
            elif u == 0:
                elem(1 - v, sa.at[(j + 1 + h) & 1], PER * (1 - h) + PER - 1)
            else:
                elem(1 - v, sa.at[j & 1], PER * h + u - 1)
            back = 1 - h if u < 2 else 0
            grads(v, back_rows(h, u, 2), j - back, g - back, h == 0 if u == 2 else None)

        @pl.when(h == 1)
        def _():
            wnext(g + STEPS)

        if ph == 1:
            @pl.when(j + 1 < STEPS)
            def _():
                @pl.when(h == 0)
                def _():
                    a_load(j + 1).start()

                @pl.when(h == 1)
                def _():
                    a_load(j + 1).wait()

        hooks(2 * g + h)

    def turn(rr):
        qv[rr, :] = acc[rr, :].astype(BF16)

    for ph in range(2):
        hv[1] = zero
        gv[0] = zero
        dv[0] = zero
        if ph == 0:
            av[1] = zero
        lax.fori_loop(0, 2 * STEPS, lambda q, _, ph=ph: (half(ph, q), 0)[1], 0)
        last = ph * STEPS + STEPS - 1
        if ph == 0:
            a_load(0).start()
            sa[1, TOK - MC:, :] = zero
            elem(1, av.at[1], None)
        else:
            elem(1, sa.at[1], 2 * PER - 1)
        grads(0, rows(2 * PER - 2), STEPS - 1, last, None)
        grads(1, rows(2 * PER - 1), STEPS - 1, last, None)
        if ph == 0:
            pcopy = pltpu.make_async_copy(x0, pv, psem.at[0])
            pcopy.start()
            sweep(turn)
            pcopy.wait()
            a_load(0).wait()
        else:
            hooks(2 * BLOCKS)
            sweep(turn)
            pltpu.make_async_copy(qv, dx_out, psem.at[1]).start()

    def drain(n, _):
        hooks(n)
        return 0

    lax.fori_loop(2 * BLOCKS + 1, 2 * BLOCKS + TAIL, drain, 0)

    for k, (peers, place) in enumerate(((row, dxi), (plane, 2 * zb + yb))):
        copies = [pltpu.make_async_remote_copy(
            src_ref=sqv.at[k], dst_ref=sqr.at[k, place], send_sem=nsend.at[k, m], recv_sem=nrecv.at[k, m],
            device_id=peer, device_id_type=MESH) for m, peer in enumerate(peers)]
        sqr[k, place] = sqv[k]
        for cp in copies:
            cp.start()
        for cp in copies:
            cp.wait()
        sqv[k + 1] = (sqr[k, 0] + sqr[k, 1]) + (sqr[k, 2] + sqr[k, 3])
    sq_out[...] = sqv[2]
    pltpu.make_async_copy(qv, dx_out, psem.at[1]).wait()


def run_main(x_rows, g_rows, w_one, w_two, w_three, w_four):
    vm = pltpu.VMEM
    dma = pltpu.SemaphoreType.DMA
    out = jax.ShapeDtypeStruct
    scratch = [
        vm((TOK, DM), BF16), vm((TOK, DM), BF16), vm((TOK, DM), F32),
        vm((3, DM, BC), BF16), vm((3, BC, DM), BF16),
        vm((2, MC, BC), BF16), vm((2, MC, BC), BF16), vm((2, MC, BC), BF16), vm((2, MC, BC), BF16),
        vm((2, TOK, BC), BF16),
        vm((2, DM, 2 * BC), F32), vm((3, DM, BC), F32), vm((NS, DM // 2, BC), F32),
        vm((NS, DM // 4, BC), F32), vm((NS, DM // 8, BC), F32), vm((2, BC, DM // 8), F32),
        vm((3, 8, 128), F32), vm((2, 4, 8, 128), F32),
        dma((8, NS)), dma((8, NS)), dma((NS,)), dma((2, 3)), dma((2,)), dma((2,)), dma((2, 3)), dma((2, 3)),
    ]
    hbm = pl.BlockSpec(memory_space=pl.ANY)
    return pl.pallas_call(
        main_kernel,
        out_shape=(out((2, DM, DF), F32), out((2, DF, DM), F32), *[out((LATE // 3, DM // 8, BC), F32)] * 3,
                   out((TOK, DM), BF16), out((8, 128), F32), out((STEPS, TOK, BC), BF16)),
        in_specs=[hbm] * 6,
        out_specs=(hbm,) * 6 + (pl.BlockSpec(memory_space=pltpu.VMEM), hbm),
        scratch_shapes=scratch,
        compiler_params=pltpu.CompilerParams(
            collective_id=0, has_side_effects=True, vmem_limit_bytes=63 * 2 ** 20),
        cost_estimate=pl.CostEstimate(flops=2 * 11 * TOK * DM * DF, bytes_accessed=250_000_000,
                                      transcendentals=3 * TOK * DF),
        name='grad_main',
    )(x_rows, g_rows, w_three, w_one, w_four, w_two)


def scaled(x, scale):
    return x * (1.0 / 16) * scale


def early_kernel(scale, ta_ref, tb_ref, oa_ref, ob_ref):
    oa_ref[...] = scaled(ta_ref[0], scale[0])
    ob_ref[...] = scaled(tb_ref[0], scale[0])


def write_early(ta, tb, scale, ph, steps):
    n = 8
    wide = steps * BC
    return pl.pallas_call(
        early_kernel,
        out_shape=(jax.ShapeDtypeStruct((DM, DF), F32), jax.ShapeDtypeStruct((DF, DM), F32)),
        grid=(n,),
        in_specs=[pl.BlockSpec(memory_space=pltpu.SMEM),
                  pl.BlockSpec((1, DM // n, wide), lambda j: (ph, j, 0)),
                  pl.BlockSpec((1, wide // n, DM), lambda j: (ph, j, 0))],
        out_specs=(pl.BlockSpec((DM // n, wide), lambda j: (j, 0)), pl.BlockSpec((wide // n, DM), lambda j: (j, 0))),
        cost_estimate=pl.CostEstimate(flops=50_000_000 * steps, bytes_accessed=16 * DM * BC * steps,
                                      transcendentals=0),
        name='write_early',
    )(scale, ta, tb)


def copy_kernel(src, dst):
    dst[...] = src[...]


def copy_rows(x):
    spec = pl.BlockSpec((TOK // 4, DM), lambda j: (j, 0))
    return pl.pallas_call(
        copy_kernel, out_shape=jax.ShapeDtypeStruct(x.shape, x.dtype), grid=(4,), in_specs=[spec], out_specs=spec,
        cost_estimate=pl.CostEstimate(flops=20_000_000, bytes_accessed=4 * TOK * DM, transcendentals=0),
        name='copy_rows',
    )(x)


def late_kernel(far, mine, scale, m0, m1, m2, oa_in, ob_in, oa, ob, held, buf_a, buf_b, isem, sem):
    dxi = lax.axis_index('dx')
    holder = dxi % 2 if mine else 1 - dxi % 2
    bits = (dxi // 2, lax.axis_index('dy'), lax.axis_index('dz'))
    loads = [[pltpu.make_async_copy(ref.at[h], held.at[group, h], isem.at[group, h]) for h in range(2)]
             for group, ref in enumerate((m0, m1, m2))]
    for pair in loads:
        for cp in pair:
            cp.start()

    def put(core):
        copies = []
        for group in range(3):
            place = [bits[(EARLY + group + core + k) % 3] for k in range(3)]
            for h in range(2):
                loads[group][h].wait()
                start = (place[0] + far) % 2 * 512 + (place[1] + h) % 2 * 256
                cut = pl.ds(pl.multiple_of(start, 256), 256)
                for m in range(LATE // 3):
                    n = len(copies)
                    col = ((EARLY + group) % STEPS + 3 * m) * BC
                    for f in range(2):
                        at = pl.multiple_of((f + place[2]) % 2 * 128, 128)
                        x = scaled(held[group, h, f, m], scale[0])
                        if core == 0:
                            buf_a[n, pl.ds(at, 128), :] = x
                        else:
                            buf_b[n, :, pl.ds(at, 128)] = x.T
                    if core == 0:
                        cp = pltpu.make_async_copy(buf_a.at[n], oa.at[cut, pl.ds(col, BC)], sem.at[n])
                    else:
                        cp = pltpu.make_async_copy(buf_b.at[n], ob.at[pl.ds(col, BC), cut], sem.at[n])
                    cp.start()
                    copies.append(cp)
        for cp in copies:
            cp.wait()

    for core in range(2):
        @pl.when(holder == core)
        def _():
            put(core)


def join_kernel(*refs):
    own, got, out, (held, isem, osem) = refs[:3], refs[3:6], refs[6:9], refs[9:]
    loads = [[pltpu.make_async_copy(part[n], held.at[n, k], isem.at[n, k]) for k, part in enumerate((own, got))]
             for n in range(3)]
    stores = [pltpu.make_async_copy(held.at[n], out[n], osem.at[n]) for n in range(3)]
    for pair in loads:
        for cp in pair:
            cp.start()
    for n in range(3):
        for cp in loads[n]:
            cp.wait()
        stores[n].start()
    for cp in stores:
        cp.wait()


def join(own, got):
    hbm = pl.BlockSpec(memory_space=pl.ANY)
    shape = (2,) + own[0].shape
    return pl.pallas_call(
        join_kernel,
        out_shape=(jax.ShapeDtypeStruct(shape, F32),) * 3,
        in_specs=[hbm] * 6,
        out_specs=(hbm,) * 3,
        scratch_shapes=[pltpu.VMEM((3,) + shape, F32), pltpu.SemaphoreType.DMA((3, 2)), pltpu.SemaphoreType.DMA((3,))],
        cost_estimate=pl.CostEstimate(flops=5_000_000, bytes_accessed=24 * math.prod(shape), transcendentals=0),
        name='join',
    )(*own, *got)


def write_late(scale, parts, outs, far, mine):
    n = 2 * LATE
    hbm = pl.BlockSpec(memory_space=pl.ANY)
    return pl.pallas_call(
        functools.partial(late_kernel, far, mine),
        out_shape=(jax.ShapeDtypeStruct((DM, DF), F32), jax.ShapeDtypeStruct((DF, DM), F32)),
        in_specs=[pl.BlockSpec(memory_space=pltpu.SMEM)] + [hbm] * 5,
        out_specs=(hbm, hbm),
        scratch_shapes=[pltpu.VMEM((3, 2, 2, LATE // 3, DM // 8, BC), F32),
                        pltpu.VMEM((n, DM // 4, BC), F32), pltpu.VMEM((n, BC, DM // 4), F32),
                        pltpu.SemaphoreType.DMA((3, 2)), pltpu.SemaphoreType.DMA((n,))],
        input_output_aliases={4: 0, 5: 1},
        cost_estimate=pl.CostEstimate(flops=30_000_000, bytes_accessed=4 * DM * BC * LATE, transcendentals=0),
        name='write_late',
    )(scale, *parts, *outs)


def solution(mesh):
    row_spec = P(AXES, None)
    masks = (2, 4, 8)

    def hop(x, group, k):
        first = (EARLY + group) % 3
        pairs = [(r, r ^ masks[(first + r % 2 + k) % 3]) for r in range(16)]
        return lax.ppermute(x, AXES, pairs)

    def per_device(x_rows, g_rows, w_one, w_two, w_three, w_four, clip_norm):
        ta, tb, *late, dx_rows, sq, _ = run_main(x_rows, g_rows, w_one, w_two, w_three, w_four)
        scale = jnp.minimum(1.0, clip_norm / jnp.sqrt(jnp.sum(sq)))
        swap = [(r, r ^ 1) for r in range(16)]
        groups = range(3)
        got = [hop(late[n], n, 2) for n in groups]
        dx_rows = copy_rows(dx_rows)
        got, dx_rows = lax.optimization_barrier((got, dx_rows))
        pair = join(late, got)
        got = [hop(pair[n], n, 1) for n in groups]
        g_one, g_two = write_early(ta, tb, scale, 1, EARLY - STEPS)
        got, g_one, g_two = lax.optimization_barrier((got, g_one, g_two))
        near = join(pair, got)
        far = [hop(near[n], n, 0) for n in groups]
        other = [lax.ppermute(near[n], AXES, swap) for n in groups]
        g_three, g_four = write_early(ta, tb, scale, 0, STEPS)
        outs = write_late(scale, near, (g_one, g_two), 0, True)
        other, outs, g_three, g_four = lax.optimization_barrier((other, outs, g_three, g_four))
        outs = write_late(scale, other, outs, 0, False)
        far, outs = lax.optimization_barrier((far, outs))
        other = [lax.ppermute(far[n], AXES, swap) for n in groups]
        outs = write_late(scale, far, outs, 1, True)
        other, outs = lax.optimization_barrier((other, outs))
        g_one, g_two = write_late(scale, other, outs, 1, False)
        return g_one, g_two, g_three, g_four, dx_rows

    return jax.shard_map(per_device, mesh=mesh, in_specs=(row_spec, row_spec, P(), P(), P(), P(), P()),
                         out_specs=(P(), P(), P(), P(), row_spec), check_vma=False)
```
